128 devices in a mesh: gx: 16 (over x_hi, z, core), gy: 8 (over y, x_lo).
Axes of the slice: x: 4 (x_hi: 2, x_lo: 2; x = x_hi * 2 + x_lo), y: 4, z: 4, core: 2. Of those that a mesh axis runs over, the one named last changes fastest.
Arguments:
- signal: float32 [131072, 128], P(('gx', 'gy')), may hold values from -6 to 6
- filter_taps: float32 [131072, 128], P(('gx', 'gy')), may hold values from -6 to 6
- grad_out: float32 [131072, 128], P(('gx', 'gy')), may hold values from -0.015625 to 0.015625
Outputs:
- grad_signal: float32 [131072, 128], P(('gx', 'gy'))
- grad_filter: float32 [131072, 128], P(('gx', 'gy'))
The draws below stay inside these ranges and needn't reach their ends.
All inputs are finite; a program needn't handle non-finite values.
Results may differ from the reference program's by a relative error of at most 0.000098.
Values sent between devices are 32-bit elements; how exact they have to be, the bound alone decides.
No kernel may reach another device: no remote copies, remote signals or barrier semaphores. Data moves between devices by JAX's collectives and lax.ppermute only.
A program may use at most 128 MiB of HBM per device.

```python
import jax
import jax.numpy as jnp

CH = 128
SEQ = 131072


def level_of(rng, dims, cuts, smallest, largest):
    factor_of, own = 1.0, jax.random.fold_in(rng, 6)
    for axis_at, blocks in cuts:
        heights = jnp.exp(jax.random.uniform(jax.random.fold_in(own, axis_at), (blocks,), jnp.float32, smallest / len(cuts), largest / len(cuts)))
        factor_of = factor_of * jnp.repeat(heights, dims[axis_at] // blocks).reshape([-1 if axis == axis_at else 1 for axis in range(len(dims))])
    return factor_of


def gaussian(stream_key, dims, width, bound, pieces=(), held_as=jnp.bfloat16):
    gain = level_of(stream_key, dims, pieces, -0.22, 0.18) if pieces else 1.0
    result = jax.random.normal(stream_key, dims, jnp.float32) * width * gain
    return jnp.minimum(jnp.maximum(result, -bound), bound).astype(held_as)


def setup_inputs(seed: int = 0) -> dict:
    keys = jax.random.split(jax.random.key(seed), 4)
    return {
        "signal": gaussian(keys[0], (SEQ, CH), 1.0, 6.0, ((0, 128),), jnp.float32),
        "filter_taps": gaussian(keys[1], (SEQ, CH), 1.0, 6.0, ((0, 128),), jnp.float32),
        "grad_out": gaussian(keys[2], (SEQ, CH), SEQ ** -0.5, 0.015625, ((0, 128),), jnp.float32),
    }


def reference(signal, filter_taps, grad_out):
    length = signal.shape[0]
    padded_length = 2 * length
    spec_signal = jnp.fft.fft(signal, n=padded_length, axis=0)
    spec_filter = jnp.fft.fft(filter_taps, n=padded_length, axis=0)
    spec_grad = jnp.fft.fft(grad_out, n=padded_length, axis=0)
    prod_signal = jnp.conj(spec_filter) * spec_grad
    prod_filter = jnp.conj(spec_signal) * spec_grad
    grad_signal = jnp.fft.ifft(prod_signal, axis=0)[:length].real.astype(jnp.float32)
    grad_filter = jnp.fft.ifft(prod_filter, axis=0)[:length].real.astype(jnp.float32)
    return grad_signal, grad_filter
```

```python
import jax
import jax.numpy as jnp
import numpy as np
from jax import lax
from jax.experimental import pallas as pl
from jax.experimental.pallas import tpu as pltpu
from jax.sharding import PartitionSpec as P

f32 = jnp.float32
bf16 = jnp.bfloat16
AXES = ("gx", "gy")
B = 128
RADIX = 8


def turn(count):
    angle = 2.0 * np.pi * count
    return np.cos(angle), np.sin(angle)


def halves(matrix):
    high = matrix.astype(np.float32).astype(jnp.bfloat16)
    low = (matrix - high.astype(np.float64)).astype(np.float32).astype(jnp.bfloat16)
    return high, low


def tables(length):
    index = np.arange(B)
    cosine, sine = turn((index[:, None] * index[None, :] % B) / B)
    left = np.block([[cosine, sine], [-sine, cosine]])
    left_back = np.block([[cosine, -sine], [sine, cosine]])
    packed = []
    for matrix in (left, left_back):
        high, low = halves(matrix)
        packed.append(np.concatenate([high, high, low], axis=1))
    for matrix in (left.T, left_back.T):
        high, low = halves(matrix)
        packed.append(np.concatenate([high, low], axis=0))
    m = np.arange(RADIX)
    inner = index[None, :, None] * (m[:, None, None] + 0.25) / (RADIX * B) * np.ones((1, 1, B))
    inner = np.stack(turn(inner), axis=1)
    outer = index[None, None, :] * (RADIX * index[None, :, None] + m[:, None, None] + 0.25) / length
    outer = np.stack(turn(outer), axis=1)
    return packed, inner.astype(np.float32), outer.astype(np.float32)


def scaled(pair, constant):
    real, imaginary = pair
    cosine, sine = constant
    return real * cosine - imaginary * sine, real * sine + imaginary * cosine


def spread(rows):
    root = np.float32(np.sqrt(0.5))
    out = [None] * RADIX
    halfway = [rows[a + 4] * root for a in range(4)]
    for odd in range(2):
        points = []
        for a in range(4):
            if odd:
                pair = (rows[a] - halfway[a], halfway[a])
            else:
                pair = (rows[a] + halfway[a], -halfway[a])
            if a:
                cosine, sine = turn(-a * (odd + 0.25) / RADIX)
                pair = scaled(pair, (np.float32(cosine), np.float32(sine)))
            points.append(pair)
        (r0, i0), (r1, i1), (r2, i2), (r3, i3) = points
        er, ei, fr, fi = r0 + r2, i0 + i2, r0 - r2, i0 - i2
        gr, gi, hr, hi = r1 + r3, i1 + i3, r1 - r3, i1 - i3
        out[odd] = (er + gr, ei + gi)
        out[2 + odd] = (fr + hi, fi - hr)
        out[4 + odd] = (er - gr, ei - gi)
        out[6 + odd] = (fr - hi, fi + hr)
    return out


def gather_real(parts):
    root = np.float32(np.sqrt(0.5))
    rows = [None] * RADIX
    both = []
    for odd in range(2):
        (r0, i0), (r1, i1), (r2, i2), (r3, i3) = (parts[2 * n + odd] for n in range(4))
        er, ei, fr, fi = r0 + r2, i0 + i2, r0 - r2, i0 - i2
        gr, gi, hr, hi = r1 + r3, i1 + i3, r1 - r3, i1 - i3
        points = [(er + gr, ei + gi), (fr - hi, fi + hr), (er - gr, ei - gi), (fr + hi, fi - hr)]
        for a in range(1, 4):
            cosine, sine = turn(a * (odd + 0.25) / RADIX)
            points[a] = scaled(points[a], (np.float32(cosine), np.float32(sine)))
        both.append(points)
    for a in range(4):
        (er, ei), (fr, fi) = both[0][a], both[1][a]
        rows[a] = er + fr
        rows[a + 4] = ((er - fr) - (ei - fi)) * root
    return rows


def split(value):
    high = value.astype(bf16)
    return high, (value - high.astype(f32)).astype(bf16)


def times(pattern, left, right):
    return jnp.dot(left, right, preferred_element_type=f32)


def left_product(matrix_ref, data):
    return jnp.dot(matrix_ref[:, : 4 * B], data, preferred_element_type=f32) + jnp.dot(
        matrix_ref[:, 4 * B :], data[: 2 * B], preferred_element_type=f32
    )


def right_product(high, low, matrix_ref):
    top = matrix_ref[: 2 * B, :]
    return (
        jnp.dot(high, top, preferred_element_type=f32)
        + jnp.dot(low, top, preferred_element_type=f32)
        + jnp.dot(high, matrix_ref[2 * B :, :], preferred_element_type=f32)
    )


def pack_kernel(signal_ref, filter_ref, grad_ref, out_ref):
    for q, ref in enumerate((signal_ref, filter_ref, grad_ref)):
        for r in range(ref.shape[0] // B):
            out_ref[:, 8 * q + r, :] = ref[r * B : (r + 1) * B, :].T


def unpack_kernel(in_ref, first_ref, second_ref):
    for q, ref in enumerate((first_ref, second_ref)):
        for r in range(ref.shape[0] // B):
            ref[r * B : (r + 1) * B, :] = in_ref[:, 8 * q + r, :].T


CHUNK = 16


def channel_kernel(scale, in_ref, left_ref, left_back_ref, right_ref, right_back_ref, inner_ref, outer_ref, out_ref, stage, back):
    blocks = in_ref.shape[0] // RADIX
    for q in range(3):
        for chunk in range(B // CHUNK):
            rows = []
            for a in range(RADIX):
                start = a * blocks + chunk * (CHUNK // 8)
                rows.append(in_ref[start : start + CHUNK // 8, 8 * q : 8 * q + 8, :].reshape(CHUNK, B))
            here = slice(chunk * CHUNK, (chunk + 1) * CHUNK)
            for m, pair in enumerate(spread(rows)):
                real, imaginary = scaled(pair, (inner_ref[m, 0, here, :], -inner_ref[m, 1, here, :]))
                lanes = slice((m % 2) * B, (m % 2 + 1) * B)
                for part, value in enumerate((real, imaginary)):
                    high, low = split(value)
                    at = part * B + chunk * CHUNK
                    stage[q, m // 2, at : at + CHUNK, lanes] = high
                    stage[q, m // 2, 2 * B + at : 2 * B + at + CHUNK, lanes] = low
    for pair_at in range(RADIX // 2):
        spectra = []
        for q in range(3):
            mixed = left_product(left_ref, stage[q, pair_at])
            turned = []
            for half in range(2):
                m = 2 * pair_at + half
                lanes = slice(half * B, (half + 1) * B)
                real, imaginary = scaled(
                    (mixed[:B, lanes], mixed[B:, lanes]), (outer_ref[m, 0], -outer_ref[m, 1])
                )
                turned.append(jnp.concatenate([real, imaginary], axis=1))
            high, low = split(jnp.concatenate(turned, axis=0))
            spectra.append(right_product(high, low, right_ref))
        grad_re, grad_im = spectra[2][:, :B], spectra[2][:, B:]
        for q in range(2):
            other_re, other_im = spectra[1 - q][:, :B], spectra[1 - q][:, B:]
            product = jnp.concatenate(
                [other_re * grad_re + other_im * grad_im, other_re * grad_im - other_im * grad_re], axis=1
            )
            high, low = split(product)
            mixed = right_product(high, low, right_back_ref)
            columns = []
            for half in range(2):
                m = 2 * pair_at + half
                real, imaginary = scaled(
                    (mixed[half * B : (half + 1) * B, :B], mixed[half * B : (half + 1) * B, B:]),
                    (outer_ref[m, 0], outer_ref[m, 1]),
                )
                columns.append(jnp.concatenate([real, imaginary], axis=0))
            high, low = split(jnp.concatenate(columns, axis=1))
            back[q, pair_at] = left_product(left_back_ref, jnp.concatenate([high, low], axis=0))
    for q in range(2):
        for chunk in range(B // CHUNK):
            here = slice(chunk * CHUNK, (chunk + 1) * CHUNK)
            parts = []
            for m in range(RADIX):
                lanes = slice((m % 2) * B, (m % 2 + 1) * B)
                at = chunk * CHUNK
                pair = (back[q, m // 2, at : at + CHUNK, lanes], back[q, m // 2, B + at : B + at + CHUNK, lanes])
                parts.append(scaled(pair, (inner_ref[m, 0, here, :], inner_ref[m, 1, here, :])))
            for a, row in enumerate(gather_real(parts)):
                start = a * blocks + chunk * (CHUNK // 8)
                out_ref[start : start + CHUNK // 8, 8 * q : 8 * q + 8, :] = (row * scale).reshape(CHUNK // 8, 8, B)


def whole(count):
    return [pl.BlockSpec(memory_space=pltpu.VMEM)] * count


def call(kernel, outs, count, name, scratch=(), interpret=False):
    specs = whole(len(outs))
    return pl.pallas_call(
        kernel,
        out_shape=outs,
        in_specs=whole(count),
        out_specs=specs,
        scratch_shapes=list(scratch),
        name=name,
        interpret=interpret,
        compiler_params=pltpu.CompilerParams(vmem_limit_bytes=48 * 1024 * 1024),
    )


def pack(signal, filter_taps, grad_out, interpret=False):
    shape = jax.ShapeDtypeStruct((B, 24, B), f32)
    return call(pack_kernel, [shape], 3, "pack", interpret=interpret)(signal, filter_taps, grad_out)[0]


def transform(received, interpret=False):
    blocks = received.shape[0]
    length = blocks * 8 * B
    packed, inner, outer = tables(length)
    constants = [jnp.asarray(table) for table in packed] + [jnp.asarray(inner), jnp.asarray(outer)]

    def kernel(*refs):
        channel_kernel(np.float32(1.0 / length), *refs)

    shape = jax.ShapeDtypeStruct((blocks, 16, B), f32)
    scratch = [pltpu.VMEM((3, RADIX // 2, 4 * B, 2 * B), bf16), pltpu.VMEM((2, RADIX // 2, 2 * B, 2 * B), f32)]
    return call(kernel, [shape], 7, "channel", scratch, interpret)(received, *constants)[0]


def unpack(received, interpret=False):
    shape = jax.ShapeDtypeStruct((8 * B, B), f32)
    return call(unpack_kernel, [shape, shape], 1, "unpack", interpret=interpret)(received)


def exchange(array):
    return lax.all_to_all(array, AXES, split_axis=0, concat_axis=0, tiled=True)


def shards(signal, filter_taps, grad_out):
    received = exchange(pack(signal, filter_taps, grad_out))
    returned = exchange(transform(received))
    first, second = unpack(returned)
    return first, second


def solution(mesh):
    return jax.shard_map(
        shards,
        mesh=mesh,
        in_specs=(P(AXES, None), P(AXES, None), P(AXES, None)),
        out_specs=(P(AXES, None), P(AXES, None)),
        check_vma=False,
    )
```

```python
import jax
import jax.numpy as jnp
import numpy as np
from jax import lax
from jax.experimental import pallas as pl
from jax.experimental.pallas import tpu as pltpu
from jax.sharding import PartitionSpec as P

f32 = jnp.float32
bf16 = jnp.bfloat16
AXES = ("gx", "gy")
B = 128
RADIX = 8


def turn(count):
    angle = 2.0 * np.pi * count
    return np.cos(angle), np.sin(angle)


def halves(matrix):
    high = matrix.astype(np.float32).astype(jnp.bfloat16)
    low = (matrix - high.astype(np.float64)).astype(np.float32).astype(jnp.bfloat16)
    return high, low


def tables(length):
    index = np.arange(B)
    cosine, sine = turn((index[:, None] * index[None, :] % B) / B)
    left = np.block([[cosine, sine], [-sine, cosine]])
    left_back = np.block([[cosine, -sine], [sine, cosine]])
    packed = []
    for matrix in (left, left_back):
        high, low = halves(matrix)
        packed.append(np.concatenate([high, high, low], axis=1))
    for matrix in (left.T, left_back.T):
        high, low = halves(matrix)
        packed.append(np.concatenate([high, low], axis=0))
    m = np.arange(RADIX)
    position = B * index[:, None] + index[None, :]
    inner = np.stack(turn(position[None] * (m[:, None, None] + 0.25) / length), axis=1)
    outer = np.stack(turn(RADIX * index[:, None] * index[None, :] / length))
    return packed, inner.astype(np.float32), outer.astype(np.float32)


def scaled(pair, constant):
    real, imaginary = pair
    cosine, sine = constant
    return real * cosine - imaginary * sine, real * sine + imaginary * cosine


def spread(rows):
    root = np.float32(np.sqrt(0.5))
    out = [None] * RADIX
    halfway = [rows[a + 4] * root for a in range(4)]
    for odd in range(2):
        points = []
        for a in range(4):
            if odd:
                pair = (rows[a] - halfway[a], halfway[a])
            else:
                pair = (rows[a] + halfway[a], -halfway[a])
            if a:
                cosine, sine = turn(-a * (odd + 0.25) / RADIX)
                pair = scaled(pair, (np.float32(cosine), np.float32(sine)))
            points.append(pair)
        (r0, i0), (r1, i1), (r2, i2), (r3, i3) = points
        er, ei, fr, fi = r0 + r2, i0 + i2, r0 - r2, i0 - i2
        gr, gi, hr, hi = r1 + r3, i1 + i3, r1 - r3, i1 - i3
        out[odd] = (er + gr, ei + gi)
        out[2 + odd] = (fr + hi, fi - hr)
        out[4 + odd] = (er - gr, ei - gi)
        out[6 + odd] = (fr - hi, fi + hr)
    return out


def gather_real(parts):
    root = np.float32(np.sqrt(0.5))
    rows = [None] * RADIX
    both = []
    for odd in range(2):
        (r0, i0), (r1, i1), (r2, i2), (r3, i3) = (parts[2 * n + odd] for n in range(4))
        er, ei, fr, fi = r0 + r2, i0 + i2, r0 - r2, i0 - i2
        gr, gi, hr, hi = r1 + r3, i1 + i3, r1 - r3, i1 - i3
        points = [(er + gr, ei + gi), (fr - hi, fi + hr), (er - gr, ei - gi), (fr + hi, fi - hr)]
        for a in range(1, 4):
            cosine, sine = turn(a * (odd + 0.25) / RADIX)
            points[a] = scaled(points[a], (np.float32(cosine), np.float32(sine)))
        both.append(points)
    for a in range(4):
        (er, ei), (fr, fi) = both[0][a], both[1][a]
        rows[a] = er + fr
        rows[a + 4] = ((er - fr) - (ei - fi)) * root
    return rows


def split(value):
    high = value.astype(bf16)
    return high, (value - high.astype(f32)).astype(bf16)


def left_product(matrix_ref, data):
    return jnp.dot(matrix_ref[:, : 4 * B], data, preferred_element_type=f32) + jnp.dot(
        matrix_ref[:, 4 * B :], data[: 2 * B], preferred_element_type=f32
    )


def right_product(high, low, matrix_ref):
    top = matrix_ref[: 2 * B, :]
    return (
        jnp.dot(high, top, preferred_element_type=f32)
        + jnp.dot(low, top, preferred_element_type=f32)
        + jnp.dot(high, matrix_ref[2 * B :, :], preferred_element_type=f32)
    )


def pack_kernel(signal_ref, filter_ref, grad_ref, out_ref, held, arrived):
    refs = (signal_ref, filter_ref, grad_ref)
    rows = signal_ref.shape[0] // B
    copies = []
    for r in range(rows):
        for q, ref in enumerate(refs):
            here = pl.ds(r * B, B)
            copies.append(pltpu.make_async_copy(ref.at[here], held.at[q, here], arrived.at[q, r]))
            copies[-1].start()
    for r in range(rows):
        for q in range(3):
            copies[3 * r + q].wait()
            out_ref[:, 8 * q + r, :] = held[q, r * B : (r + 1) * B, :].T


def unpack_kernel(in_ref, first_ref, second_ref, held, left):
    copies = []
    for q, ref in enumerate((first_ref, second_ref)):
        for r in range(ref.shape[0] // B):
            held[q, r * B : (r + 1) * B, :] = in_ref[:, 8 * q + r, :].T
            here = pl.ds(r * B, B)
            copies.append(pltpu.make_async_copy(held.at[q, here], ref.at[here], left.at[q, r]))
            copies[-1].start()
    for copy in copies:
        copy.wait()


CHUNK = 16


def channel_kernel(scale, in_ref, left_ref, left_back_ref, right_ref, right_back_ref, inner_ref, outer_ref, out_ref, stage, back):
    blocks = in_ref.shape[0] // RADIX
    for q in range(3):
        for chunk in range(B // CHUNK):
            rows = []
            for a in range(RADIX):
                start = a * blocks + chunk * (CHUNK // 8)
                rows.append(in_ref[start : start + CHUNK // 8, 8 * q : 8 * q + 8, :].reshape(CHUNK, B))
            here = slice(chunk * CHUNK, (chunk + 1) * CHUNK)
            for m, pair in enumerate(spread(rows)):
                real, imaginary = scaled(pair, (inner_ref[m, 0, here, :], -inner_ref[m, 1, here, :]))
                lanes = slice((m % 2) * B, (m % 2 + 1) * B)
                for part, value in enumerate((real, imaginary)):
                    high, low = split(value)
                    at = part * B + chunk * CHUNK
                    stage[q, m // 2, at : at + CHUNK, lanes] = high
                    stage[q, m // 2, 2 * B + at : 2 * B + at + CHUNK, lanes] = low
    for pair_at in range(RADIX // 2):
        spectra = []
        for q in range(3):
            mixed = left_product(left_ref, stage[q, pair_at])
            turned = []
            for half in range(2):
                m = 2 * pair_at + half
                lanes = slice(half * B, (half + 1) * B)
                real, imaginary = scaled(
                    (mixed[:B, lanes], mixed[B:, lanes]), (outer_ref[0], -outer_ref[1])
                )
                turned.append(jnp.concatenate([real, imaginary], axis=1))
            high, low = split(jnp.concatenate(turned, axis=0))
            spectra.append(right_product(high, low, right_ref))
        grad_re, grad_im = spectra[2][:, :B], spectra[2][:, B:]
        for q in range(2):
            other_re, other_im = spectra[1 - q][:, :B], spectra[1 - q][:, B:]
            product = jnp.concatenate(
                [other_re * grad_re + other_im * grad_im, other_re * grad_im - other_im * grad_re], axis=1
            )
            high, low = split(product)
            mixed = right_product(high, low, right_back_ref)
            columns = []
            for half in range(2):
                m = 2 * pair_at + half
                real, imaginary = scaled(
                    (mixed[half * B : (half + 1) * B, :B], mixed[half * B : (half + 1) * B, B:]),
                    (outer_ref[0], outer_ref[1]),
                )
                columns.append(jnp.concatenate([real, imaginary], axis=0))
            high, low = split(jnp.concatenate(columns, axis=1))
            back[q, pair_at] = left_product(left_back_ref, jnp.concatenate([high, low], axis=0))
    for q in range(2):
        for chunk in range(B // CHUNK):
            here = slice(chunk * CHUNK, (chunk + 1) * CHUNK)
            parts = []
            for m in range(RADIX):
                lanes = slice((m % 2) * B, (m % 2 + 1) * B)
                at = chunk * CHUNK
                pair = (back[q, m // 2, at : at + CHUNK, lanes], back[q, m // 2, B + at : B + at + CHUNK, lanes])
                parts.append(scaled(pair, (inner_ref[m, 0, here, :], inner_ref[m, 1, here, :])))
            for a, row in enumerate(gather_real(parts)):
                start = a * blocks + chunk * (CHUNK // 8)
                out_ref[start : start + CHUNK // 8, 8 * q : 8 * q + 8, :] = (row * scale).reshape(CHUNK // 8, 8, B)


def call(kernel, out_shape, in_spaces, out_spaces, name, scratch, interpret):
    return pl.pallas_call(
        kernel,
        out_shape=out_shape,
        in_specs=[pl.BlockSpec(memory_space=space) for space in in_spaces],
        out_specs=[pl.BlockSpec(memory_space=space) for space in out_spaces],
        scratch_shapes=scratch,
        name=name,
        interpret=interpret,
        compiler_params=pltpu.CompilerParams(vmem_limit_bytes=48 * 1024 * 1024),
    )


def pack(signal, filter_taps, grad_out, interpret=False):
    rows = signal.shape[0]
    shape = jax.ShapeDtypeStruct((B, 24, B), f32)
    scratch = [pltpu.VMEM((3, rows, B), f32), pltpu.SemaphoreType.DMA((3, rows // B))]
    packed = call(pack_kernel, [shape], [pltpu.HBM] * 3, [pltpu.VMEM], "pack", scratch, interpret)
    inputs = (signal, filter_taps, grad_out)
    if not interpret:
        inputs = [pltpu.with_memory_space_constraint(x, pltpu.HBM) for x in inputs]
    return packed(*inputs)[0]


def transform(received, interpret=False):
    blocks = received.shape[0]
    length = blocks * 8 * B
    packed, inner, outer = tables(length)
    constants = [jnp.asarray(table) for table in packed] + [jnp.asarray(inner), jnp.asarray(outer)]

    def kernel(*refs):
        channel_kernel(np.float32(1.0 / length), *refs)

    shape = jax.ShapeDtypeStruct((blocks, 16, B), f32)
    scratch = [pltpu.VMEM((3, RADIX // 2, 4 * B, 2 * B), bf16), pltpu.VMEM((2, RADIX // 2, 2 * B, 2 * B), f32)]
    return call(kernel, [shape], [pltpu.VMEM] * 7, [pltpu.VMEM], "channel", scratch, interpret)(received, *constants)[0]


def unpack(received, interpret=False):
    rows = 8 * B
    shape = jax.ShapeDtypeStruct((rows, B), f32)
    scratch = [pltpu.VMEM((2, rows, B), f32), pltpu.SemaphoreType.DMA((2, rows // B))]
    return call(unpack_kernel, [shape] * 2, [pltpu.VMEM], [pltpu.HBM] * 2, "unpack", scratch, interpret)(received)


def exchange(array):
    return lax.all_to_all(array, AXES, split_axis=0, concat_axis=0, tiled=True)


def shards(signal, filter_taps, grad_out):
    received = exchange(pack(signal, filter_taps, grad_out))
    returned = exchange(transform(received))
    first, second = unpack(returned)
    return first, second


def solution(mesh):
    return jax.shard_map(
        shards,
        mesh=mesh,
        in_specs=(P(AXES, None), P(AXES, None), P(AXES, None)),
        out_specs=(P(AXES, None), P(AXES, None)),
        check_vma=False,
    )
```

```python
import jax
import jax.numpy as jnp
import numpy as np
from jax import lax
from jax.experimental import pallas as pl
from jax.experimental.pallas import tpu as pltpu
from jax.sharding import PartitionSpec as P

f32 = jnp.float32
bf16 = jnp.bfloat16
AXES = ("gx", "gy")
B = 128
RADIX = 8


def turn(count):
    angle = 2.0 * np.pi * count
    return np.cos(angle), np.sin(angle)


def halves(matrix):
    high = matrix.astype(np.float32).astype(jnp.bfloat16)
    low = (matrix - high.astype(np.float64)).astype(np.float32).astype(jnp.bfloat16)
    return high, low


def tables(length):
    index = np.arange(B)
    cosine, sine = turn((index[:, None] * index[None, :] % B) / B)
    left = np.block([[cosine, sine], [-sine, cosine]])
    left_back = np.block([[cosine, -sine], [sine, cosine]])
    packed = []
    for matrix in (left, left_back):
        high, low = halves(matrix)
        packed.append(np.concatenate([high, high, low], axis=1))
    for matrix in (left.T, left_back.T):
        high, low = halves(matrix)
        packed.append(np.concatenate([high, low], axis=0))
    m = np.arange(RADIX)
    position = B * index[:, None] + index[None, :]
    inner = np.stack(turn(position[None] * (m[:, None, None] + 0.25) / length), axis=1)
    outer = np.stack(turn(RADIX * index[:, None] * index[None, :] / length))
    return packed, inner.astype(np.float32), outer.astype(np.float32)


def scaled(pair, constant):
    real, imaginary = pair
    cosine, sine = constant
    return real * cosine - imaginary * sine, real * sine + imaginary * cosine


def spread(rows):
    root = np.float32(np.sqrt(0.5))
    out = [None] * RADIX
    halfway = [rows[a + 4] * root for a in range(4)]
    for odd in range(2):
        points = []
        for a in range(4):
            if odd:
                pair = (rows[a] - halfway[a], halfway[a])
            else:
                pair = (rows[a] + halfway[a], -halfway[a])
            if a:
                cosine, sine = turn(-a * (odd + 0.25) / RADIX)
                pair = scaled(pair, (np.float32(cosine), np.float32(sine)))
            points.append(pair)
        (r0, i0), (r1, i1), (r2, i2), (r3, i3) = points
        er, ei, fr, fi = r0 + r2, i0 + i2, r0 - r2, i0 - i2
        gr, gi, hr, hi = r1 + r3, i1 + i3, r1 - r3, i1 - i3
        out[odd] = (er + gr, ei + gi)
        out[2 + odd] = (fr + hi, fi - hr)
        out[4 + odd] = (er - gr, ei - gi)
        out[6 + odd] = (fr - hi, fi + hr)
    return out


def gather_real(parts):
    root = np.float32(np.sqrt(0.5))
    rows = [None] * RADIX
    both = []
    for odd in range(2):
        (r0, i0), (r1, i1), (r2, i2), (r3, i3) = (parts[2 * n + odd] for n in range(4))
        er, ei, fr, fi = r0 + r2, i0 + i2, r0 - r2, i0 - i2
        gr, gi, hr, hi = r1 + r3, i1 + i3, r1 - r3, i1 - i3
        points = [(er + gr, ei + gi), (fr - hi, fi + hr), (er - gr, ei - gi), (fr + hi, fi - hr)]
        for a in range(1, 4):
            cosine, sine = turn(a * (odd + 0.25) / RADIX)
            points[a] = scaled(points[a], (np.float32(cosine), np.float32(sine)))
        both.append(points)
    for a in range(4):
        (er, ei), (fr, fi) = both[0][a], both[1][a]
        rows[a] = er + fr
        rows[a + 4] = ((er - fr) - (ei - fi)) * root
    return rows


def split(value):
    high = value.astype(bf16)
    return high, (value - high.astype(f32)).astype(bf16)


def left_product(matrix_ref, data):
    return jnp.dot(matrix_ref[:, : 4 * B], data, preferred_element_type=f32) + jnp.dot(
        matrix_ref[:, 4 * B :], data[: 2 * B], preferred_element_type=f32
    )


def right_product(high, low, matrix_ref):
    top = matrix_ref[: 2 * B, :]
    return (
        jnp.dot(high, top, preferred_element_type=f32)
        + jnp.dot(low, top, preferred_element_type=f32)
        + jnp.dot(high, matrix_ref[2 * B :, :], preferred_element_type=f32)
    )


def pack_kernel(signal_ref, filter_ref, grad_ref, out_ref, held, arrived):
    copies = []
    for q, ref in enumerate((signal_ref, filter_ref, grad_ref)):
        copies.append(pltpu.make_async_copy(ref, held.at[q], arrived.at[q]))
        copies[-1].start()
    for q, copy in enumerate(copies):
        copy.wait()
        for r in range(8):
            out_ref[pl.ds(8 * q + r, B, stride=24), :] = held[q, r * B : (r + 1) * B, :].T


def unpack_kernel(in_ref, first_ref, second_ref, held, left):
    copies = []
    for q, ref in enumerate((first_ref, second_ref)):
        for r in range(ref.shape[0] // B):
            held[q, r * B : (r + 1) * B, :] = in_ref[pl.ds(8 * q + r, B, stride=16), :].T
            here = pl.ds(r * B, B)
            copies.append(pltpu.make_async_copy(held.at[q, here], ref.at[here], left.at[q, r]))
            copies[-1].start()
    for copy in copies:
        copy.wait()


CHUNK = 16
LAG = 2
PAIRS = RADIX // 2
CHUNKS = B // CHUNK


def interleaved(tasks, fillers):
    done, order = {}, []

    def ready(needs, lag):
        return all(need in done and len(order) - done[need] > lag for need in needs)

    def emit(name, run):
        run()
        done[name] = len(order)
        order.append(name)

    tasks, fillers = list(tasks), list(fillers)
    while tasks or fillers:
        for lag in range(LAG, -1, -1):
            found = next((task for task in tasks if ready(task[1], lag)), None)
            if found:
                break
        if found:
            tasks.remove(found)
            emit(found[0], found[2])
        filler = next((one for one in fillers if ready(one[1], 0)), None)
        if filler:
            fillers.remove(filler)
            emit(filler[0], filler[2])


def channel_kernel(scale, in_ref, left_ref, left_back_ref, right_ref, right_back_ref, inner_ref, outer_ref, out_ref, stage, back):
    blocks = in_ref.shape[0] // RADIX
    mixed, spectra, returned = {}, {}, {}

    def load(q, chunk):
        rows = []
        for a in range(RADIX):
            start = a * blocks + chunk * (CHUNK // 8)
            rows.append(in_ref[start : start + CHUNK // 8, 8 * q : 8 * q + 8, :].reshape(CHUNK, B))
        here = slice(chunk * CHUNK, (chunk + 1) * CHUNK)
        for m, pair in enumerate(spread(rows)):
            parts = scaled(pair, (inner_ref[m, 0, here, :], -inner_ref[m, 1, here, :]))
            lanes = slice((m % 2) * B, (m % 2 + 1) * B)
            for part, value in enumerate(parts):
                high, low = split(value)
                at = part * B + chunk * CHUNK
                stage[q, m // 2, at : at + CHUNK, lanes] = high
                stage[q, m // 2, 2 * B + at : 2 * B + at + CHUNK, lanes] = low

    def first(q, pair_at):
        mixed[q, pair_at] = left_product(left_ref, stage[q, pair_at])

    def second(q, pair_at):
        value = mixed.pop((q, pair_at))
        turned = []
        for half in range(2):
            lanes = slice(half * B, (half + 1) * B)
            parts = scaled((value[:B, lanes], value[B:, lanes]), (outer_ref[0], -outer_ref[1]))
            turned.append(jnp.concatenate(parts, axis=1))
        high, low = split(jnp.concatenate(turned, axis=0))
        spectra[q, pair_at] = right_product(high, low, right_ref)

    def third(q, pair_at):
        grad, other = spectra[2, pair_at], spectra[1 - q, pair_at]
        grad_re, grad_im, other_re, other_im = grad[:, :B], grad[:, B:], other[:, :B], other[:, B:]
        real = other_re * grad_re + other_im * grad_im
        imaginary = other_re * grad_im - other_im * grad_re
        high, low = split(jnp.concatenate([real, imaginary], axis=1))
        returned[q, pair_at] = right_product(high, low, right_back_ref)

    def fourth(q, pair_at):
        value = returned.pop((q, pair_at))
        columns = []
        for half in range(2):
            rows = slice(half * B, (half + 1) * B)
            parts = scaled((value[rows, :B], value[rows, B:]), (outer_ref[0], outer_ref[1]))
            columns.append(jnp.concatenate(parts, axis=0))
        high, low = split(jnp.concatenate(columns, axis=1))
        back[q, pair_at] = left_product(left_back_ref, jnp.concatenate([high, low], axis=0))

    def store(q, chunk):
        at = chunk * CHUNK
        parts = []
        for m in range(RADIX):
            lanes = slice((m % 2) * B, (m % 2 + 1) * B)
            pair = (back[q, m // 2, at : at + CHUNK, lanes], back[q, m // 2, B + at : B + at + CHUNK, lanes])
            table = (inner_ref[m, 0, at : at + CHUNK, :], inner_ref[m, 1, at : at + CHUNK, :])
            parts.append(scaled(pair, table))
        for a, row in enumerate(gather_real(parts)):
            start = a * blocks + chunk * (CHUNK // 8)
            out_ref[start : start + CHUNK // 8, 8 * q : 8 * q + 8, :] = (row * scale).reshape(CHUNK // 8, 8, B)

    def task(run, q, at, needs):
        return (run.__name__, q, at), needs, lambda: run(q, at)

    tasks, fillers = [], []
    for q in (2, 0, 1):
        loads = [("load", q, chunk) for chunk in range(CHUNKS)]
        fillers += [task(load, q, chunk, []) for chunk in range(CHUNKS)]
        for pair_at in range(PAIRS):
            tasks.append(task(second, q, pair_at, [("first", q, pair_at)]))
            tasks.append(task(first, q, pair_at, loads))
        if q != 2:
            for pair_at in range(PAIRS):
                out = 1 - q
                tasks.append(task(fourth, out, pair_at, [("third", out, pair_at)]))
                needs = [("second", 2, pair_at), ("second", q, pair_at)]
                tasks.append(task(third, out, pair_at, needs))
            needs = [("fourth", out, pair_at) for pair_at in range(PAIRS)]
            fillers += [task(store, out, chunk, needs) for chunk in range(CHUNKS)]
    interleaved(tasks, fillers)


def call(kernel, out_shape, in_spaces, out_spaces, name, scratch, interpret):
    return pl.pallas_call(
        kernel,
        out_shape=out_shape,
        in_specs=[pl.BlockSpec(memory_space=space) for space in in_spaces],
        out_specs=[pl.BlockSpec(memory_space=space) for space in out_spaces],
        scratch_shapes=scratch,
        name=name,
        interpret=interpret,
        compiler_params=pltpu.CompilerParams(vmem_limit_bytes=48 * 1024 * 1024),
    )


def pack(signal, filter_taps, grad_out, interpret=False):
    rows = signal.shape[0]
    shape = jax.ShapeDtypeStruct((24 * B, B), f32)
    scratch = [pltpu.VMEM((3, rows, B), f32), pltpu.SemaphoreType.DMA((3,))]
    packed = call(pack_kernel, [shape], [pltpu.HBM] * 3, [pltpu.VMEM], "pack", scratch, interpret)
    inputs = (signal, filter_taps, grad_out)
    if not interpret:
        inputs = [pltpu.with_memory_space_constraint(x, pltpu.HBM) for x in inputs]
    return packed(*inputs)[0].reshape(B, 24, B)


def transform(received, interpret=False):
    blocks = received.shape[0]
    length = blocks * 8 * B
    packed, inner, outer = tables(length)
    constants = [jnp.asarray(table) for table in packed] + [jnp.asarray(inner), jnp.asarray(outer)]

    def kernel(*refs):
        channel_kernel(np.float32(1.0 / length), *refs)

    shape = jax.ShapeDtypeStruct((blocks, 16, B), f32)
    scratch = [pltpu.VMEM((3, RADIX // 2, 4 * B, 2 * B), bf16), pltpu.VMEM((2, RADIX // 2, 2 * B, 2 * B), f32)]
    return call(kernel, [shape], [pltpu.VMEM] * 7, [pltpu.VMEM], "channel", scratch, interpret)(received, *constants)[0]


def unpack(received, interpret=False):
    rows = 8 * B
    shape = jax.ShapeDtypeStruct((rows, B), f32)
    scratch = [pltpu.VMEM((2, rows, B), f32), pltpu.SemaphoreType.DMA((2, rows // B))]
    return call(unpack_kernel, [shape] * 2, [pltpu.VMEM], [pltpu.HBM] * 2, "unpack", scratch, interpret)(received.reshape(16 * B, B))


def exchange(array):
    return lax.all_to_all(array, AXES, split_axis=0, concat_axis=0, tiled=True)


def shards(signal, filter_taps, grad_out):
    received = exchange(pack(signal, filter_taps, grad_out))
    returned = exchange(transform(received))
    first, second = unpack(returned)
    return first, second


def solution(mesh):
    return jax.shard_map(
        shards,
        mesh=mesh,
        in_specs=(P(AXES, None), P(AXES, None), P(AXES, None)),
        out_specs=(P(AXES, None), P(AXES, None)),
        check_vma=False,
    )
```

```python
import jax
import jax.numpy as jnp
import numpy as np
from jax import lax
from jax.experimental import pallas as pl
from jax.experimental.pallas import tpu as pltpu
from jax.sharding import PartitionSpec as P

f32 = jnp.float32
bf16 = jnp.bfloat16
AXES = ("gx", "gy")
B = 128
RADIX = 8


def turn(count):
    angle = 2.0 * np.pi * count
    return np.cos(angle), np.sin(angle)


def halves(matrix):
    high = matrix.astype(np.float32).astype(jnp.bfloat16)
    low = (matrix - high.astype(np.float64)).astype(np.float32).astype(jnp.bfloat16)
    return high, low


def tables(length):
    index = np.arange(B)
    cosine, sine = turn((index[:, None] * index[None, :] % B) / B)
    left = np.block([[cosine, sine], [-sine, cosine]])
    left_back = np.block([[cosine, -sine], [sine, cosine]])
    scale = 1.0 / length
    packed = []
    for matrix in (left, left_back * scale):
        high, low = halves(matrix)
        packed.append(np.concatenate([high, low], axis=1))
    for matrix in (left.T, left_back.T):
        high, low = halves(matrix)
        packed.append(np.concatenate([high, low], axis=0))
    m = np.arange(RADIX)
    position = B * index[:, None] + index[None, :]
    inner = np.stack(turn(position[None] * (m[:, None, None] + 0.25) / length), axis=1)
    outer = np.stack(turn(RADIX * index[:, None] * index[None, :] / length))
    return packed, inner.astype(np.float32), outer.astype(np.float32)


def scaled(pair, constant):
    real, imaginary = pair
    cosine, sine = constant
    return real * cosine - imaginary * sine, real * sine + imaginary * cosine


def butterfly(points, sign):
    (r0, i0), (r1, i1), (r2, i2), (r3, i3) = points
    er, ei, fr, fi = r0 + r2, i0 + i2, r0 - r2, i0 - i2
    gr, gi, hr, hi = r1 + r3, i1 + i3, r1 - r3, i1 - i3
    middle = [(fr + hi, fi - hr), (fr - hi, fi + hr)]
    return (er + gr, ei + gi), middle[sign > 0], (er - gr, ei - gi), middle[sign < 0]


def constants_of(a, odd):
    near, far = turn(a * (odd + 0.25) / RADIX), turn((a + 4) * (odd + 0.25) / RADIX)
    return [np.float32(value) for value in (*near, *far)]


def spread(rows):
    root = np.float32(np.sqrt(0.5))
    out = [None] * RADIX
    far = rows[4] * root
    for odd in range(2):
        points = [(rows[0] - far, far) if odd else (rows[0] + far, -far)]
        for a in range(1, 4):
            cosine, sine, far_cosine, far_sine = constants_of(a, odd)
            real = rows[a] * cosine + rows[a + 4] * far_cosine
            points.append((real, rows[a] * -sine + rows[a + 4] * -far_sine))
        for n, pair in enumerate(butterfly(points, -1)):
            out[2 * n + odd] = pair
    return out


def gather_real(parts):
    root = np.float32(np.sqrt(0.5))
    even, odd = (butterfly([parts[2 * n + one] for n in range(4)], 1) for one in range(2))
    rows = [None] * RADIX
    rows[0] = even[0][0] + odd[0][0]
    rows[4] = ((even[0][0] - odd[0][0]) - (even[0][1] - odd[0][1])) * root
    for a in range(1, 4):
        first, second = constants_of(a, 0), constants_of(a, 1)
        for far in range(2):
            cosine, sine = first[2 * far : 2 * far + 2]
            other_cosine, other_sine = second[2 * far : 2 * far + 2]
            total = even[a][0] * cosine - even[a][1] * sine
            rows[a + 4 * far] = total + (odd[a][0] * other_cosine - odd[a][1] * other_sine)
    return rows


def split(value):
    high = value.astype(bf16)
    return high, (value - high.astype(f32)).astype(bf16)


def left_product(matrix_ref, data):
    high, low = data[: 2 * B], data[2 * B :]
    top = matrix_ref[:, : 2 * B]
    return (
        jnp.dot(top, high, preferred_element_type=f32)
        + jnp.dot(matrix_ref[:, 2 * B :], high, preferred_element_type=f32)
        + jnp.dot(top, low, preferred_element_type=f32)
    )


def right_product(high, low, matrix_ref):
    top = matrix_ref[: 2 * B, :]
    return (
        jnp.dot(high, top, preferred_element_type=f32)
        + jnp.dot(high, matrix_ref[2 * B :, :], preferred_element_type=f32)
        + jnp.dot(low, top, preferred_element_type=f32)
    )


def pack_kernel(signal_ref, filter_ref, grad_ref, out_ref, held, arrived):
    copies = []
    for q, ref in enumerate((signal_ref, filter_ref, grad_ref)):
        copies.append(pltpu.make_async_copy(ref, held.at[q], arrived.at[q]))
        copies[-1].start()
    for q, copy in enumerate(copies):
        copy.wait()
        for r in range(8):
            out_ref[pl.ds(8 * q + r, B, stride=24), :] = held[q, r * B : (r + 1) * B, :].T


def unpack_kernel(in_ref, first_ref, second_ref, held, left):
    copies = []
    for q, ref in enumerate((first_ref, second_ref)):
        for r in range(ref.shape[0] // B):
            held[q, r * B : (r + 1) * B, :] = in_ref[pl.ds(8 * q + r, B, stride=16), :].T
            here = pl.ds(r * B, B)
            copies.append(pltpu.make_async_copy(held.at[q, here], ref.at[here], left.at[q, r]))
            copies[-1].start()
    for copy in copies:
        copy.wait()


CHUNK = 16
WIDE = 2
PAIRS = RADIX // WIDE
CHUNKS = B // CHUNK


def interleaved(tasks, fillers):
    done = set()
    while tasks or fillers:
        for names in (tasks, fillers):
            found = next((one for one in names if done.issuperset(one[1])), None)
            if found:
                names.remove(found)
                found[2]()
                done.add(found[0])


def channel_kernel(in_ref, left_ref, left_back_ref, right_ref, right_back_ref, inner_ref, outer_ref, out_ref, stage, back):
    blocks = in_ref.shape[0] // RADIX
    mixed, spectra, returned = {}, {}, {}

    def load(q, chunk):
        rows = []
        for a in range(RADIX):
            start = a * blocks + chunk * (CHUNK // 8)
            rows.append(in_ref[start : start + CHUNK // 8, 8 * q : 8 * q + 8, :].reshape(CHUNK, B))
        here = slice(chunk * CHUNK, (chunk + 1) * CHUNK)
        for m, pair in enumerate(spread(rows)):
            parts = scaled(pair, (inner_ref[m, 0, here, :], -inner_ref[m, 1, here, :]))
            lanes = slice(m % WIDE * B, (m % WIDE + 1) * B)
            for part, value in enumerate(parts):
                high, low = split(value)
                at = part * B + chunk * CHUNK
                stage[q, m // WIDE, at : at + CHUNK, lanes] = high
                stage[q, m // WIDE, 2 * B + at : 2 * B + at + CHUNK, lanes] = low

    def first(q, pair_at):
        mixed[q, pair_at] = left_product(left_ref, stage[q, pair_at])

    def second(q, pair_at):
        value = mixed.pop((q, pair_at))
        turned = []
        for half in range(WIDE):
            lanes = slice(half * B, (half + 1) * B)
            parts = scaled((value[:B, lanes], value[B:, lanes]), (outer_ref[0], -outer_ref[1]))
            turned.append(jnp.concatenate(parts, axis=1))
        high, low = split(jnp.concatenate(turned, axis=0))
        spectra[q, pair_at] = right_product(high, low, right_ref)

    def third(q, pair_at):
        grad, other = spectra[2, pair_at], spectra[1 - q, pair_at]
        grad_re, grad_im, other_re, other_im = grad[:, :B], grad[:, B:], other[:, :B], other[:, B:]
        real = other_re * grad_re + other_im * grad_im
        imaginary = other_re * grad_im - other_im * grad_re
        high, low = split(jnp.concatenate([real, imaginary], axis=1))
        returned[q, pair_at] = right_product(high, low, right_back_ref)

    def fourth(q, pair_at):
        value = returned.pop((q, pair_at))
        columns = []
        for half in range(WIDE):
            rows = slice(half * B, (half + 1) * B)
            parts = scaled((value[rows, :B], value[rows, B:]), (outer_ref[0], outer_ref[1]))
            columns.append(jnp.concatenate(parts, axis=0))
        high, low = split(jnp.concatenate(columns, axis=1))
        back[q, pair_at] = left_product(left_back_ref, jnp.concatenate([high, low], axis=0))

    def store(q, chunk):
        at = chunk * CHUNK
        parts = []
        for m in range(RADIX):
            lanes = slice(m % WIDE * B, (m % WIDE + 1) * B)
            pair = (back[q, m // WIDE, at : at + CHUNK, lanes], back[q, m // WIDE, B + at : B + at + CHUNK, lanes])
            table = (inner_ref[m, 0, at : at + CHUNK, :], inner_ref[m, 1, at : at + CHUNK, :])
            parts.append(scaled(pair, table))
        for a, row in enumerate(gather_real(parts)):
            start = a * blocks + chunk * (CHUNK // 8)
            out_ref[start : start + CHUNK // 8, 8 * q : 8 * q + 8, :] = row.reshape(CHUNK // 8, 8, B)

    def task(run, q, at, needs):
        return (run.__name__, q, at), needs, lambda: run(q, at)

    tasks, fillers = [], []
    for q in (2, 0, 1):
        loads = [("load", q, chunk) for chunk in range(CHUNKS)]
        fillers += [task(load, q, chunk, []) for chunk in range(CHUNKS)]
        for pair_at in range(PAIRS):
            tasks.append(task(second, q, pair_at, [("first", q, pair_at)]))
            tasks.append(task(first, q, pair_at, loads))
        if q != 2:
            for pair_at in range(PAIRS):
                out = 1 - q
                tasks.append(task(fourth, out, pair_at, [("third", out, pair_at)]))
                needs = [("second", 2, pair_at), ("second", q, pair_at)]
                tasks.append(task(third, out, pair_at, needs))
            needs = [("fourth", out, pair_at) for pair_at in range(PAIRS)]
            fillers += [task(store, out, chunk, needs) for chunk in range(CHUNKS)]
    interleaved(tasks, fillers)


def call(kernel, out_shape, in_spaces, out_spaces, name, scratch, interpret):
    return pl.pallas_call(
        kernel,
        out_shape=out_shape,
        in_specs=[pl.BlockSpec(memory_space=space) for space in in_spaces],
        out_specs=[pl.BlockSpec(memory_space=space) for space in out_spaces],
        scratch_shapes=scratch,
        name=name,
        interpret=interpret,
        compiler_params=pltpu.CompilerParams(vmem_limit_bytes=48 * 1024 * 1024),
    )


def pack(signal, filter_taps, grad_out, interpret=False):
    rows = signal.shape[0]
    shape = jax.ShapeDtypeStruct((24 * B, B), f32)
    scratch = [pltpu.VMEM((3, rows, B), f32), pltpu.SemaphoreType.DMA((3,))]
    packed = call(pack_kernel, [shape], [pltpu.HBM] * 3, [pltpu.VMEM], "pack", scratch, interpret)
    inputs = (signal, filter_taps, grad_out)
    if not interpret:
        inputs = [pltpu.with_memory_space_constraint(x, pltpu.HBM) for x in inputs]
    return packed(*inputs)[0].reshape(B, 24, B)


def transform(received, interpret=False):
    blocks = received.shape[0]
    length = blocks * 8 * B
    packed, inner, outer = tables(length)
    constants = [jnp.asarray(table) for table in packed] + [jnp.asarray(inner), jnp.asarray(outer)]

    shape = jax.ShapeDtypeStruct((blocks, 16, B), f32)
    scratch = [pltpu.VMEM((3, PAIRS, 4 * B, WIDE * B), bf16), pltpu.VMEM((2, PAIRS, 2 * B, WIDE * B), f32)]
    return call(channel_kernel, [shape], [pltpu.VMEM] * 7, [pltpu.VMEM], "channel", scratch, interpret)(received, *constants)[0]


def unpack(received, interpret=False):
    rows = 8 * B
    shape = jax.ShapeDtypeStruct((rows, B), f32)
    scratch = [pltpu.VMEM((2, rows, B), f32), pltpu.SemaphoreType.DMA((2, rows // B))]
    return call(unpack_kernel, [shape] * 2, [pltpu.VMEM], [pltpu.HBM] * 2, "unpack", scratch, interpret)(received.reshape(16 * B, B))


def exchange(array):
    return lax.all_to_all(array, AXES, split_axis=0, concat_axis=0, tiled=True)


def shards(signal, filter_taps, grad_out):
    received = exchange(pack(signal, filter_taps, grad_out))
    returned = exchange(transform(received))
    first, second = unpack(returned)
    return first, second


def solution(mesh):
    return jax.shard_map(
        shards,
        mesh=mesh,
        in_specs=(P(AXES, None), P(AXES, None), P(AXES, None)),
        out_specs=(P(AXES, None), P(AXES, None)),
        check_vma=False,
    )
```

```python
import jax
import jax.numpy as jnp
import numpy as np
from jax import lax
from jax.experimental import pallas as pl
from jax.experimental.pallas import tpu as pltpu
from jax.sharding import PartitionSpec as P

f32 = jnp.float32
bf16 = jnp.bfloat16
AXES = ("gx", "gy")
B = 128
RADIX = 8


def turn(count):
    angle = 2.0 * np.pi * count
    return np.cos(angle), np.sin(angle)


def halves(matrix):
    high = matrix.astype(np.float32).astype(jnp.bfloat16)
    low = (matrix - high.astype(np.float64)).astype(np.float32).astype(jnp.bfloat16)
    return high, low


def tables(length):
    index = np.arange(B)
    cosine, sine = turn(index[None, :] * (4 * index[:, None] + 1) % (4 * B) / (4 * B))
    high, low = halves(np.concatenate([cosine, -sine], axis=0))
    packed = [np.concatenate([high, high, low], axis=1)]
    high, low = halves(np.concatenate([cosine.T, -sine.T], axis=1) / length)
    packed.append(np.concatenate([high, low], axis=1))
    cosine, sine = turn((index[:, None] * index[None, :] % B) / B)
    for matrix in (np.block([[cosine, -sine], [sine, cosine]]), np.block([[cosine, sine], [-sine, cosine]])):
        high, low = halves(matrix)
        packed.append(np.concatenate([high, low], axis=0))
    r = np.arange(RADIX)
    position = B * r[:, None, None] + index[None, None, :]
    inner = np.stack(turn(position * (4 * index[None, :, None] + 1) % (4 * length) / (4 * length)), axis=1)
    outer = np.concatenate(turn(r[:, None] * index[None, :] / (RADIX * B)))
    return packed, inner.astype(np.float32), outer.astype(np.float32)


def scaled(pair, constant):
    real, imaginary = pair
    cosine, sine = constant
    return real * cosine - imaginary * sine, real * sine + imaginary * cosine


def butterfly(points, sign):
    (r0, i0), (r1, i1), (r2, i2), (r3, i3) = points
    er, ei, fr, fi = r0 + r2, i0 + i2, r0 - r2, i0 - i2
    gr, gi, hr, hi = r1 + r3, i1 + i3, r1 - r3, i1 - i3
    middle = [(fr + hi, fi - hr), (fr - hi, fi + hr)]
    return (er + gr, ei + gi), middle[sign > 0], (er - gr, ei - gi), middle[sign < 0]


def eighths(points, sign):
    root = np.float32(np.sqrt(0.5))
    even, odd = butterfly(points[0::2], sign), butterfly(points[1::2], sign)
    (r1, i1), (r2, i2), (r3, i3) = odd[1:]
    if sign < 0:
        turned = [odd[0], ((r1 + i1) * root, (i1 - r1) * root), (i2, -r2), ((i3 - r3) * root, -(i3 + r3) * root)]
    else:
        turned = [odd[0], ((r1 - i1) * root, (i1 + r1) * root), (-i2, r2), (-(r3 + i3) * root, (r3 - i3) * root)]
    plus = [(e[0] + o[0], e[1] + o[1]) for e, o in zip(even, turned)]
    return plus + [(e[0] - o[0], e[1] - o[1]) for e, o in zip(even, turned)]


def split(value):
    high = value.astype(bf16)
    return high, (value - high.astype(f32)).astype(bf16)


def right_product(high, low, matrix_ref):
    top = matrix_ref[: 2 * B, :]
    return (
        jnp.dot(high, top, preferred_element_type=f32)
        + jnp.dot(high, matrix_ref[2 * B :, :], preferred_element_type=f32)
        + jnp.dot(low, top, preferred_element_type=f32)
    )


def pack_kernel(signal_ref, filter_ref, grad_ref, out_ref, held, arrived):
    copies = []
    for q, ref in enumerate((signal_ref, filter_ref, grad_ref)):
        copies.append(pltpu.make_async_copy(ref, held.at[q], arrived.at[q]))
        copies[-1].start()
    for q, copy in enumerate(copies):
        copy.wait()
        for r in range(8):
            out_ref[pl.ds(8 * q + r, B, stride=24), :] = held[q, r * B : (r + 1) * B, :].T


def unpack_kernel(in_ref, first_ref, second_ref, held, left):
    copies = []
    for q, ref in enumerate((first_ref, second_ref)):
        for r in range(ref.shape[0] // B):
            held[q, r * B : (r + 1) * B, :] = in_ref[pl.ds(8 * q + r, B, stride=16), :].T
            here = pl.ds(r * B, B)
            copies.append(pltpu.make_async_copy(held.at[q, here], ref.at[here], left.at[q, r]))
            copies[-1].start()
    for copy in copies:
        copy.wait()


CHUNK = 16
PAIRS = RADIX // 2
CHUNKS = B // CHUNK


def interleaved(tasks, fillers):
    done = set()
    while tasks or fillers:
        for names in (tasks, fillers, fillers):
            found = next((one for one in names if done.issuperset(one[1])), None)
            if found:
                names.remove(found)
                found[2]()
                done.add(found[0])


def channel_kernel(
    in_ref, left_ref, left_back_ref, right_ref, right_back_ref, inner_ref, outer_ref, out_ref,
    start, mixed, high_ref, low_ref, returned, last,
):
    spectra = {}

    def lanes_of(n):
        return slice(n % 2 * B, (n % 2 + 1) * B)

    def outer(m, sign):
        return outer_ref[m : m + 1, :], sign * outer_ref[RADIX + m : RADIX + m + 1, :]

    def enter(q, d):
        high, low = split(in_ref[pl.ds(8 * q + d, B, stride=24), :])
        start[q, d // 2, :B, lanes_of(d)] = high
        start[q, d // 2, B:, lanes_of(d)] = low

    def first(q, pair_at):
        data = start[q, pair_at]
        mixed[q, pair_at] = jnp.dot(left_ref[:, : 2 * B], data, preferred_element_type=f32) + jnp.dot(
            left_ref[:, 2 * B :], data[:B], preferred_element_type=f32
        )

    def middle(q, chunk):
        here = slice(chunk * CHUNK, (chunk + 1) * CHUNK)
        under = slice(B + chunk * CHUNK, B + (chunk + 1) * CHUNK)
        points = []
        for d in range(RADIX):
            pair = mixed[q, d // 2, here, lanes_of(d)], mixed[q, d // 2, under, lanes_of(d)]
            points.append(scaled(pair, (inner_ref[d, 0, here, :], -inner_ref[d, 1, here, :])))
        for m, pair in enumerate(eighths(points, -1)):
            if m:
                pair = scaled(pair, outer(m, -1))
            for part, value in enumerate(pair):
                high, low = split(value)
                rows, lanes = slice(m * B + chunk * CHUNK, m * B + (chunk + 1) * CHUNK), lanes_of(part)
                high_ref[q, rows, lanes] = high
                low_ref[q, rows, lanes] = low

    def second(q, pair_at):
        rows = slice(pair_at * 2 * B, (pair_at + 1) * 2 * B)
        spectra[q, pair_at] = right_product(high_ref[q, rows, :], low_ref[q, rows, :], right_ref)

    def third(q, pair_at):
        grad, other = spectra[2, pair_at], spectra[1 - q, pair_at]
        grad_re, grad_im, other_re, other_im = grad[:, :B], grad[:, B:], other[:, :B], other[:, B:]
        real = other_re * grad_re + other_im * grad_im
        imaginary = other_re * grad_im - other_im * grad_re
        high, low = split(jnp.concatenate([real, imaginary], axis=1))
        returned[q, pair_at] = right_product(high, low, right_back_ref)

    def middle_back(q, chunk):
        here = slice(chunk * CHUNK, (chunk + 1) * CHUNK)
        points = []
        for m in range(RADIX):
            rows = slice(m % 2 * B + chunk * CHUNK, m % 2 * B + (chunk + 1) * CHUNK)
            pair = returned[q, m // 2, rows, :B], returned[q, m // 2, rows, B:]
            points.append(scaled(pair, outer(m, 1)) if m else pair)
        for d, pair in enumerate(eighths(points, 1)):
            pair = scaled(pair, (inner_ref[d, 0, here, :], inner_ref[d, 1, here, :]))
            for part, value in enumerate(pair):
                high, low = split(value)
                at = part * B + chunk * CHUNK
                last[q, d // 2, at : at + CHUNK, lanes_of(d)] = high
                last[q, d // 2, 2 * B + at : 2 * B + at + CHUNK, lanes_of(d)] = low

    def fourth(q, pair_at):
        high, low = last[q, pair_at, : 2 * B], last[q, pair_at, 2 * B :]
        top = left_back_ref[:, : 2 * B]
        result = (
            jnp.dot(top, high, preferred_element_type=f32)
            + jnp.dot(left_back_ref[:, 2 * B :], high, preferred_element_type=f32)
            + jnp.dot(top, low, preferred_element_type=f32)
        )
        for d in (2 * pair_at, 2 * pair_at + 1):
            out_ref[pl.ds(8 * q + d, B, stride=16), :] = result[:, lanes_of(d)]

    def every(run, q, needs, count=PAIRS):
        return [((run.__name__, q, at), needs(at), lambda at=at: run(q, at)) for at in range(count)]

    def firsts(q):
        return every(first, q, lambda at: [("enter", q, 2 * at), ("enter", q, 2 * at + 1)])

    def seconds(q):
        return every(second, q, lambda at: [("middle", q, chunk) for chunk in range(CHUNKS)])

    def thirds(q):
        return every(third, q, lambda at: [("second", 2, at), ("second", 1 - q, at)])

    def fourths(q):
        return every(fourth, q, lambda at: [("middle_back", q, chunk) for chunk in range(CHUNKS)])

    def enters(q):
        return every(enter, q, lambda at: [], RADIX)

    def middles(q):
        return every(middle, q, lambda at: [("first", q, pair_at) for pair_at in range(PAIRS)], CHUNKS)

    def middles_back(q):
        return every(middle_back, q, lambda at: [("third", q, pair_at) for pair_at in range(PAIRS)], CHUNKS)

    tasks = firsts(2) + firsts(0) + seconds(2) + firsts(1) + seconds(0) + thirds(1)
    tasks += seconds(1) + thirds(0) + fourths(1) + fourths(0)
    fillers = enters(2) + enters(0) + middles(2) + enters(1) + middles(0) + middles(1)
    fillers += middles_back(1) + middles_back(0)
    interleaved(tasks, fillers)


def call(kernel, out_shape, in_spaces, out_spaces, name, scratch, interpret):
    return pl.pallas_call(
        kernel,
        out_shape=out_shape,
        in_specs=[pl.BlockSpec(memory_space=space) for space in in_spaces],
        out_specs=[pl.BlockSpec(memory_space=space) for space in out_spaces],
        scratch_shapes=scratch,
        name=name,
        interpret=interpret,
        compiler_params=pltpu.CompilerParams(vmem_limit_bytes=48 * 1024 * 1024),
    )


def pack(signal, filter_taps, grad_out, interpret=False):
    rows = signal.shape[0]
    shape = jax.ShapeDtypeStruct((24 * B, B), f32)
    scratch = [pltpu.VMEM((3, rows, B), f32), pltpu.SemaphoreType.DMA((3,))]
    packed = call(pack_kernel, [shape], [pltpu.HBM] * 3, [pltpu.VMEM], "pack", scratch, interpret)
    inputs = (signal, filter_taps, grad_out)
    if not interpret:
        inputs = [pltpu.with_memory_space_constraint(x, pltpu.HBM) for x in inputs]
    return packed(*inputs)[0].reshape(B, 24, B)


def transform(received, interpret=False):
    blocks = received.shape[0]
    length = blocks * 8 * B
    packed, inner, outer = tables(length)
    constants = [jnp.asarray(table) for table in packed] + [jnp.asarray(inner), jnp.asarray(outer)]

    shape = jax.ShapeDtypeStruct((blocks * 16, B), f32)
    scratch = [
        pltpu.VMEM((3, PAIRS, 2 * B, 2 * B), bf16),
        pltpu.VMEM((3, PAIRS, 2 * B, 2 * B), f32),
        pltpu.VMEM((3, RADIX * B, 2 * B), bf16),
        pltpu.VMEM((3, RADIX * B, 2 * B), bf16),
        pltpu.VMEM((2, PAIRS, 2 * B, 2 * B), f32),
        pltpu.VMEM((2, PAIRS, 4 * B, 2 * B), bf16),
    ]
    run = call(channel_kernel, [shape], [pltpu.VMEM] * 7, [pltpu.VMEM], "channel", scratch, interpret)
    return run(received.reshape(blocks * 24, B), *constants)[0].reshape(blocks, 16, B)


def unpack(received, interpret=False):
    rows = 8 * B
    shape = jax.ShapeDtypeStruct((rows, B), f32)
    scratch = [pltpu.VMEM((2, rows, B), f32), pltpu.SemaphoreType.DMA((2, rows // B))]
    return call(unpack_kernel, [shape] * 2, [pltpu.VMEM], [pltpu.HBM] * 2, "unpack", scratch, interpret)(received.reshape(16 * B, B))


def exchange(array):
    return lax.all_to_all(array, AXES, split_axis=0, concat_axis=0, tiled=True)


def shards(signal, filter_taps, grad_out):
    received = exchange(pack(signal, filter_taps, grad_out))
    returned = exchange(transform(received))
    first, second = unpack(returned)
    return first, second


def solution(mesh):
    return jax.shard_map(
        shards,
        mesh=mesh,
        in_specs=(P(AXES, None), P(AXES, None), P(AXES, None)),
        out_specs=(P(AXES, None), P(AXES, None)),
        check_vma=False,
    )
```

```python
import jax
import jax.numpy as jnp
import numpy as np
from jax import lax
from jax.experimental import pallas as pl
from jax.experimental.pallas import tpu as pltpu
from jax.sharding import PartitionSpec as P

f32 = jnp.float32
bf16 = jnp.bfloat16
AXES = ("gx", "gy")
B = 128
RADIX = 8


def turn(count):
    angle = 2.0 * np.pi * count
    return np.cos(angle), np.sin(angle)


def halves(matrix):
    high = matrix.astype(np.float32).astype(jnp.bfloat16)
    low = (matrix - high.astype(np.float64)).astype(np.float32).astype(jnp.bfloat16)
    return high, low


def tables(length):
    index = np.arange(B)
    cosine, sine = turn((index[:, None] * index[None, :] % B) / B)
    left = np.block([[cosine, sine], [-sine, cosine]])
    left_back = np.block([[cosine, -sine], [sine, cosine]])
    scale = 1.0 / length
    packed = []
    for matrix in (left, left_back * scale):
        high, low = halves(matrix)
        packed.append(np.concatenate([high, low], axis=1))
    for matrix in (left.T, left_back.T):
        high, low = halves(matrix)
        packed.append(np.concatenate([high, low], axis=0))
    m = np.arange(RADIX)
    position = B * index[:, None] + index[None, :]
    inner = np.stack(turn(position[None] * (m[:, None, None] + 0.25) / length), axis=1)
    outer = np.stack(turn(RADIX * index[:, None] * index[None, :] / length))
    return packed, inner.astype(np.float32), outer.astype(np.float32)


def scaled(pair, constant):
    real, imaginary = pair
    cosine, sine = constant
    return real * cosine - imaginary * sine, real * sine + imaginary * cosine


def butterfly(points, sign):
    (r0, i0), (r1, i1), (r2, i2), (r3, i3) = points
    er, ei, fr, fi = r0 + r2, i0 + i2, r0 - r2, i0 - i2
    gr, gi, hr, hi = r1 + r3, i1 + i3, r1 - r3, i1 - i3
    middle = [(fr + hi, fi - hr), (fr - hi, fi + hr)]
    return (er + gr, ei + gi), middle[sign > 0], (er - gr, ei - gi), middle[sign < 0]


def constants_of(a, odd):
    near, far = turn(a * (odd + 0.25) / RADIX), turn((a + 4) * (odd + 0.25) / RADIX)
    return [np.float32(value) for value in (*near, *far)]


def spread(rows):
    root = np.float32(np.sqrt(0.5))
    out = [None] * RADIX
    far = rows[4] * root
    for odd in range(2):
        points = [(rows[0] - far, far) if odd else (rows[0] + far, -far)]
        for a in range(1, 4):
            cosine, sine, far_cosine, far_sine = constants_of(a, odd)
            real = rows[a] * cosine + rows[a + 4] * far_cosine
            points.append((real, rows[a] * -sine + rows[a + 4] * -far_sine))
        for n, pair in enumerate(butterfly(points, -1)):
            out[2 * n + odd] = pair
    return out


def gather_real(parts):
    root = np.float32(np.sqrt(0.5))
    even, odd = (butterfly([parts[2 * n + one] for n in range(4)], 1) for one in range(2))
    rows = [None] * RADIX
    rows[0] = even[0][0] + odd[0][0]
    rows[4] = ((even[0][0] - odd[0][0]) - (even[0][1] - odd[0][1])) * root
    for a in range(1, 4):
        first, second = constants_of(a, 0), constants_of(a, 1)
        for far in range(2):
            cosine, sine = first[2 * far : 2 * far + 2]
            other_cosine, other_sine = second[2 * far : 2 * far + 2]
            total = even[a][0] * cosine - even[a][1] * sine
            rows[a + 4 * far] = total + (odd[a][0] * other_cosine - odd[a][1] * other_sine)
    return rows


def split(value):
    high = value.astype(bf16)
    return high, (value - high.astype(f32)).astype(bf16)


def left_product(matrix_ref, data):
    high, low = data[: 2 * B], data[2 * B :]
    top = matrix_ref[:, : 2 * B]
    return (
        jnp.dot(top, high, preferred_element_type=f32)
        + jnp.dot(matrix_ref[:, 2 * B :], high, preferred_element_type=f32)
        + jnp.dot(top, low, preferred_element_type=f32)
    )


def right_product(high, low, matrix_ref):
    top = matrix_ref[: 2 * B, :]
    return (
        jnp.dot(high, top, preferred_element_type=f32)
        + jnp.dot(high, matrix_ref[2 * B :, :], preferred_element_type=f32)
        + jnp.dot(low, top, preferred_element_type=f32)
    )


def pack_kernel(signal_ref, filter_ref, grad_ref, out_ref, held, arrived):
    rows = signal_ref.shape[0]
    parts = [(0, 0, rows), (1, 0, rows), (2, 0, rows // 2), (2, rows // 2, rows // 2)]
    copies = []
    for n, (q, at, size) in enumerate(parts):
        here = pl.ds(at, size)
        ref = (signal_ref, filter_ref, grad_ref)[q]
        copies.append(pltpu.make_async_copy(ref.at[here], held.at[q, here], arrived.at[n]))
        copies[-1].start()
    for copy, (q, at, size) in zip(copies, parts):
        copy.wait()
        for r in range(at // B, (at + size) // B):
            out_ref[pl.ds(8 * q + r, B, stride=24), :] = held[q, r * B : (r + 1) * B, :].T


def unpack_kernel(in_ref, first_ref, second_ref, held, left):
    copies = []
    for q, ref in enumerate((first_ref, second_ref)):
        for r in range(ref.shape[0] // B):
            held[q, r * B : (r + 1) * B, :] = in_ref[pl.ds(8 * q + r, B, stride=16), :].T
            here = pl.ds(r * B, B)
            copies.append(pltpu.make_async_copy(held.at[q, here], ref.at[here], left.at[q, r]))
            copies[-1].start()
    for copy in copies:
        copy.wait()


CHUNK = 16
WIDE = 2
PAIRS = RADIX // WIDE
CHUNKS = B // CHUNK


def interleaved(tasks, fillers):
    done = set()
    while tasks or fillers:
        for names in (tasks, fillers):
            found = next((one for one in names if done.issuperset(one[1])), None)
            if found:
                names.remove(found)
                found[2]()
                done.add(found[0])


def channel_kernel(in_ref, left_ref, left_back_ref, right_ref, right_back_ref, inner_ref, outer_ref, out_ref, stage, back):
    blocks = in_ref.shape[0] // RADIX
    mixed, spectra, returned = {}, {}, {}

    def load(q, chunk):
        rows = []
        for a in range(RADIX):
            start = a * blocks + chunk * (CHUNK // 8)
            rows.append(in_ref[start : start + CHUNK // 8, 8 * q : 8 * q + 8, :].reshape(CHUNK, B))
        here = slice(chunk * CHUNK, (chunk + 1) * CHUNK)
        for m, pair in enumerate(spread(rows)):
            parts = scaled(pair, (inner_ref[m, 0, here, :], -inner_ref[m, 1, here, :]))
            lanes = slice(m % WIDE * B, (m % WIDE + 1) * B)
            for part, value in enumerate(parts):
                high, low = split(value)
                at = part * B + chunk * CHUNK
                stage[q, m // WIDE, at : at + CHUNK, lanes] = high
                stage[q, m // WIDE, 2 * B + at : 2 * B + at + CHUNK, lanes] = low

    def first(q, pair_at):
        mixed[q, pair_at] = left_product(left_ref, stage[q, pair_at])

    def second(q, pair_at):
        value = mixed.pop((q, pair_at))
        turned = []
        for half in range(WIDE):
            lanes = slice(half * B, (half + 1) * B)
            parts = scaled((value[:B, lanes], value[B:, lanes]), (outer_ref[0], -outer_ref[1]))
            turned.append(jnp.concatenate(parts, axis=1))
        high, low = split(jnp.concatenate(turned, axis=0))
        spectra[q, pair_at] = right_product(high, low, right_ref)

    def third(q, pair_at):
        grad, other = spectra[2, pair_at], spectra[1 - q, pair_at]
        grad_re, grad_im, other_re, other_im = grad[:, :B], grad[:, B:], other[:, :B], other[:, B:]
        real = other_re * grad_re + other_im * grad_im
        imaginary = other_re * grad_im - other_im * grad_re
        high, low = split(jnp.concatenate([real, imaginary], axis=1))
        returned[q, pair_at] = right_product(high, low, right_back_ref)

    def fourth(q, pair_at):
        value = returned.pop((q, pair_at))
        columns = []
        for half in range(WIDE):
            rows = slice(half * B, (half + 1) * B)
            parts = scaled((value[rows, :B], value[rows, B:]), (outer_ref[0], outer_ref[1]))
            columns.append(jnp.concatenate(parts, axis=0))
        high, low = split(jnp.concatenate(columns, axis=1))
        back[q, pair_at] = left_product(left_back_ref, jnp.concatenate([high, low], axis=0))

    def store(q, chunk):
        at = chunk * CHUNK
        parts = []
        for m in range(RADIX):
            lanes = slice(m % WIDE * B, (m % WIDE + 1) * B)
            pair = (back[q, m // WIDE, at : at + CHUNK, lanes], back[q, m // WIDE, B + at : B + at + CHUNK, lanes])
            table = (inner_ref[m, 0, at : at + CHUNK, :], inner_ref[m, 1, at : at + CHUNK, :])
            parts.append(scaled(pair, table))
        for a, row in enumerate(gather_real(parts)):
            start = a * blocks + chunk * (CHUNK // 8)
            out_ref[start : start + CHUNK // 8, 8 * q : 8 * q + 8, :] = row.reshape(CHUNK // 8, 8, B)

    def task(run, q, at, needs):
        return (run.__name__, q, at), needs, lambda: run(q, at)

    tasks, fillers = [], []
    for q in (2, 0, 1):
        loads = [("load", q, chunk) for chunk in range(CHUNKS)]
        fillers += [task(load, q, chunk, []) for chunk in range(CHUNKS)]
        for pair_at in range(PAIRS):
            tasks.append(task(second, q, pair_at, [("first", q, pair_at)]))
            tasks.append(task(first, q, pair_at, loads))
        if q != 2:
            for pair_at in range(PAIRS):
                out = 1 - q
                tasks.append(task(fourth, out, pair_at, [("third", out, pair_at)]))
                needs = [("second", 2, pair_at), ("second", q, pair_at)]
                tasks.append(task(third, out, pair_at, needs))
            needs = [("fourth", out, pair_at) for pair_at in range(PAIRS)]
            fillers += [task(store, out, chunk, needs) for chunk in range(CHUNKS)]
    interleaved(tasks, fillers)


def call(kernel, out_shape, in_spaces, out_spaces, name, scratch, interpret):
    return pl.pallas_call(
        kernel,
        out_shape=out_shape,
        in_specs=[pl.BlockSpec(memory_space=space) for space in in_spaces],
        out_specs=[pl.BlockSpec(memory_space=space) for space in out_spaces],
        scratch_shapes=scratch,
        name=name,
        interpret=interpret,
        compiler_params=pltpu.CompilerParams(vmem_limit_bytes=48 * 1024 * 1024),
    )


def pack(signal, filter_taps, grad_out, interpret=False):
    rows = signal.shape[0]
    shape = jax.ShapeDtypeStruct((24 * B, B), f32)
    scratch = [pltpu.VMEM((3, rows, B), f32), pltpu.SemaphoreType.DMA((4,))]
    packed = call(pack_kernel, [shape], [pltpu.HBM] * 3, [pltpu.VMEM], "pack", scratch, interpret)
    inputs = (signal, filter_taps, grad_out)
    if not interpret:
        inputs = [pltpu.with_memory_space_constraint(x, pltpu.HBM) for x in inputs]
    return packed(*inputs)[0].reshape(B, 24, B)


def transform(received, interpret=False):
    blocks = received.shape[0]
    length = blocks * 8 * B
    packed, inner, outer = tables(length)
    constants = [jnp.asarray(table) for table in packed] + [jnp.asarray(inner), jnp.asarray(outer)]

    shape = jax.ShapeDtypeStruct((blocks, 16, B), f32)
    scratch = [pltpu.VMEM((3, PAIRS, 4 * B, WIDE * B), bf16), pltpu.VMEM((2, PAIRS, 2 * B, WIDE * B), f32)]
    return call(channel_kernel, [shape], [pltpu.VMEM] * 7, [pltpu.VMEM], "channel", scratch, interpret)(received, *constants)[0]


def unpack(received, interpret=False):
    rows = 8 * B
    shape = jax.ShapeDtypeStruct((rows, B), f32)
    scratch = [pltpu.VMEM((2, rows, B), f32), pltpu.SemaphoreType.DMA((2, rows // B))]
    return call(unpack_kernel, [shape] * 2, [pltpu.VMEM], [pltpu.HBM] * 2, "unpack", scratch, interpret)(received.reshape(16 * B, B))


def exchange(array):
    return lax.all_to_all(array, AXES, split_axis=0, concat_axis=0, tiled=True)


def shards(signal, filter_taps, grad_out):
    received = exchange(pack(signal, filter_taps, grad_out))
    returned = exchange(transform(received))
    first, second = unpack(returned)
    return first, second


def solution(mesh):
    return jax.shard_map(
        shards,
        mesh=mesh,
        in_specs=(P(AXES, None), P(AXES, None), P(AXES, None)),
        out_specs=(P(AXES, None), P(AXES, None)),
        check_vma=False,
    )
```
